32 devices in a mesh: wide: 16 (over z, y, x), narrow: 2 (over core).
Axes of the slice: x: 2, y: 2, z: 4, core: 2. Of those that a mesh axis runs over, the one named last changes fastest.
Arguments:
- qkv: float32 [3, 2, 1024, 1280], P(None, None, 'wide', 'narrow'), may hold values from -30 to 30
- eta: float32 [2, 1024], P('narrow', 'wide'), may hold values from 0.01 to 0.1
- fast_weights: float32 [2, 640, 3, 384], P('narrow', 'wide'), may hold values from -0.25 to 0.25
- momentum: float32 [2, 640, 3, 384], P('narrow', 'wide'), may hold values from -50 to 50
- ttt_gain: float32 [1280], P('narrow'), may hold values from 0.5 to 1.5
Outputs:
- mixed: float32 [2, 1024, 1280], P(None, 'wide', 'narrow')
- new_weights: float32 [2, 640, 3, 384], P('narrow', 'wide')
- new_momentum: float32 [2, 640, 3, 384], P('narrow', 'wide')
The draws below stay inside these ranges and needn't reach their ends.
All inputs are finite; a program needn't handle non-finite values.
Results may differ from the reference program's by a relative error of at most 0.0003.
Values sent between devices are 32-bit elements; how exact they have to be, the bound alone decides.
A program may use at most 64 MiB of HBM per device.

```python
import math
import jax
import jax.numpy as jnp
from jax import lax

D = 640
H = 384
ATT = 128
WINDOW = 128
GROUPS = 2
TOK_DEV = 64
GROUP = 1024
HEADS = 2
DMODEL = 1280


def draw_qkv(key, part):
    pieces = jax.random.split(jax.random.fold_in(key, 11), 1)
    shape = (3, GROUPS, GROUP, DMODEL)
    return jax.random.truncated_normal(pieces[0], -4.0, 4.0, shape, jnp.float32)


def draw_momentum(key, part):
    pieces = jax.random.split(jax.random.fold_in(key, 23), 2)
    shape = (HEADS, D, 3, H)
    trend = 3.0 ** (jnp.arange(D, dtype=jnp.float32) / (D - 1))
    row_scale = trend * 10.0 ** jax.random.uniform(pieces[1], (D,), jnp.float32, 0.0, 1.0)
    row_scale = row_scale[None, :, None, None]
    base = jax.random.truncated_normal(pieces[0], -4.0, 4.0, shape, jnp.float32)
    return 0.3 * base * row_scale


def levels(key, extent, cuts, smallest, high):
    def one(dim, shards_of):
        draws = jax.random.uniform(jax.random.fold_in(jax.random.fold_in(key, 6), dim), (shards_of,), jnp.float32, smallest / len(cuts), high / len(cuts))
        return jnp.repeat(jnp.exp(draws), extent[dim] // shards_of).reshape((-1,) + (1,) * (len(extent) - dim - 1))

    factor_of = one(*cuts[0])
    for cut in cuts[1:]:
        factor_of = factor_of * one(*cut)
    return factor_of


def normal_values(own_key, shape, deviation, most, cuts=(), kind=jnp.bfloat16):
    entries = deviation * jax.random.normal(own_key, shape, jnp.float32)
    if cuts:
        entries = entries * levels(own_key, shape, cuts, -0.22, 0.18)
    return jnp.clip(entries, -most, most).astype(kind)


def setup_inputs(seed: int = 0) -> dict:
    arg_keys = jax.random.split(jax.random.key(seed), 6)
    qkv = draw_qkv(jax.random.fold_in(arg_keys[5], 71), 0)
    eta = jnp.clip(jnp.exp(math.log(0.1) - 2.3025851 * jax.random.uniform(arg_keys[1], (HEADS, GROUP), jnp.float32) ** levels(arg_keys[1], (HEADS, GROUP), ((0, 2), (1, 16)), -0.2, 0.2)), 0.01, 0.1)
    fast_weights = normal_values(arg_keys[2], (HEADS, D, 3, H), D ** -0.5, 0.25, ((0, 2), (1, 16)), jnp.float32)
    momentum = draw_momentum(jax.random.fold_in(arg_keys[5], 71), 0)
    ttt_gain = jnp.clip(1.0 + 0.1 * jax.random.normal(arg_keys[4], (DMODEL,), jnp.float32), 0.5, 1.5)
    return dict(qkv=qkv, eta=eta, fast_weights=fast_weights, momentum=momentum, ttt_gain=ttt_gain)


EPSILON = 1e-06
MOMENTUM_RATE = 0.9
STEP_SIZE = 0.03
PRECISION = lax.Precision.HIGHEST

def product(left, right):
    return jnp.dot(left, right, precision=PRECISION, preferred_element_type=jnp.float32)

def memory_read(inputs, weights):
    gate_pre = product(inputs, weights[:, 0, :])
    up_pre = product(inputs, weights[:, 1, :])
    hidden = jax.nn.silu(gate_pre) * up_pre
    return product(hidden, weights[:, 2, :].T)

def memory_gradient(key_rows, value_rows, rates, weights):
    gate_pre = product(key_rows, weights[:, 0, :])
    up_pre = product(key_rows, weights[:, 1, :])
    sigmoid = jax.nn.sigmoid(gate_pre)
    gated = gate_pre * sigmoid
    hidden = gated * up_pre
    weighted = rates[:, None] * value_rows
    back = -product(weighted, weights[:, 2, :])
    gate_back = back * up_pre * sigmoid * (1.0 + gate_pre * (1.0 - sigmoid))
    up_back = back * gated
    return (weighted, hidden, gate_back, up_back)

def renormalize(weights, moment):
    spread = jnp.sqrt(lax.optimization_barrier(jnp.mean(moment * moment, axis=0)) + EPSILON)
    moved = weights - STEP_SIZE * moment / spread
    ratio = jnp.sqrt(lax.optimization_barrier(jnp.mean(weights * weights, axis=0)) + EPSILON) / jnp.sqrt(lax.optimization_barrier(jnp.mean(moved * moved, axis=0)) + EPSILON)
    return moved * ratio

def reference(qkv, eta, fast_weights, momentum, ttt_gain):
    total = GROUPS * GROUP
    head_count = DMODEL // ATT
    query_all = qkv[0].reshape(total, DMODEL)
    key_all = qkv[1].reshape(total, DMODEL)
    value_all = qkv[2].reshape(total, DMODEL)
    padding = jnp.zeros((WINDOW, DMODEL), jnp.float32)
    key_padded = jnp.concatenate([padding, key_all], axis=0)
    value_padded = jnp.concatenate([padding, value_all], axis=0)

    def attend(block):
        start = block * TOK_DEV
        query_block = lax.dynamic_slice_in_dim(query_all, start, TOK_DEV, 0).reshape(TOK_DEV, head_count, ATT)
        key_block = lax.dynamic_slice_in_dim(key_padded, start, TOK_DEV + WINDOW, 0).reshape(TOK_DEV + WINDOW, head_count, ATT)
        value_block = lax.dynamic_slice_in_dim(value_padded, start, TOK_DEV + WINDOW, 0).reshape(TOK_DEV + WINDOW, head_count, ATT)
        scores = jnp.einsum('qhe,khe->hqk', query_block, key_block, precision=PRECISION) / math.sqrt(ATT)
        query_pos = start + jnp.arange(TOK_DEV, dtype=jnp.int32)
        key_pos = start - WINDOW + jnp.arange(TOK_DEV + WINDOW, dtype=jnp.int32)
        distance = query_pos[:, None] - key_pos[None, :]
        allowed = (distance >= 0) & (distance < WINDOW) & (key_pos >= 0)[None, :]
        scores = jnp.where(allowed[None], scores, -1e+30)
        highest = lax.optimization_barrier(jnp.max(scores, axis=-1, keepdims=True))
        weights = jnp.exp(scores - highest)
        weights = weights / lax.optimization_barrier(jnp.sum(weights, axis=-1, keepdims=True))
        return jnp.einsum('hqk,khe->qhe', weights, value_block, precision=PRECISION).reshape(TOK_DEV, DMODEL)
    attended = lax.map(attend, jnp.arange(total // TOK_DEV, dtype=jnp.int32)).reshape(GROUPS, GROUP, DMODEL)
    readouts = []
    updated_list = []
    moment_list = []
    for memory in range(HEADS):
        lower = memory * D
        weights = fast_weights[memory]
        first_queries = qkv[0, 0, :, lower:lower + D]
        first_keys = qkv[1, 0, :, lower:lower + D]
        first_values = qkv[2, 0, :, lower:lower + D]
        first_read = memory_read(first_queries, weights)
        weighted, hidden, gate_back, up_back = memory_gradient(first_keys, first_values, eta[memory], weights)
        gradient = jnp.stack([product(first_keys.T, gate_back), product(first_keys.T, up_back), -product(weighted.T, hidden)], axis=1)
        moment = MOMENTUM_RATE * momentum[memory] + gradient
        updated = renormalize(weights, moment)
        second_read = memory_read(qkv[0, 1, :, lower:lower + D], updated)
        readouts.append(jnp.stack([first_read, second_read]))
        updated_list.append(updated)
        moment_list.append(moment)
    readout = jnp.concatenate(readouts, axis=-1)
    scale = jnp.sqrt(lax.optimization_barrier(jnp.mean(readout * readout, axis=-1, keepdims=True)) + EPSILON)
    mixed = attended + ttt_gain * (readout / scale)
    return (mixed, jnp.stack(updated_list), jnp.stack(moment_list))
```

```python
import functools
import math

import jax
import jax.numpy as jnp
from jax import lax
from jax.experimental import pallas as pl
from jax.experimental.pallas import tpu as pltpu
from jax.sharding import PartitionSpec as P

ATT = 128
WINDOW = 128
LANES = 128
EPSILON = 1e-06
MOMENTUM_RATE = 0.9
STEP_SIZE = 0.03
MESH = pl.DeviceIdType.MESH
F32 = jnp.float32
BF16 = jnp.bfloat16


def contract(left, right, on_left, on_right, precision=None):
    dims = (((on_left,), (on_right,)), ((), ()))
    return lax.dot_general(left, right, dims, precision=precision, preferred_element_type=F32)


def split(value):
    high = value.astype(BF16)
    return high, (value - high.astype(F32)).astype(BF16)


def times(value, high_ref, low_ref, which, on=0):
    rows = value.shape[0]
    high, low = split(value)
    both = contract(jnp.concatenate([high, low], axis=0), high_ref[which], 1, on)
    return both[:rows] + both[rows:] + contract(high, low_ref[which], 1, on)


def token_sum(left, right):
    high = left.astype(BF16).astype(F32)
    stacked = jnp.concatenate([high, high, left - high], axis=0).T.astype(BF16)
    right_high, right_low = split(right)
    return contract(stacked, jnp.concatenate([right_high, right_low, right_high], axis=0), 1, 0)


def kernel(n, plane, width, part, reach, qkv, eta, own_w, own_m, gain, mixed, new_w, new_m,
           wg, mg, grad, ra, rb, sa, sb, ra2, rb2, wfull, whi, wlo, halo, squares, read0,
           wsem, msem, a1, b1, a2, b2, hsem, qsem, ssem):
    layers = n // plane
    chunks, rows, _ = own_w.shape
    per = chunks // 3
    groups, tok = qkv.shape[1], qkv.shape[2]
    columns = qkv.shape[3]
    me = lax.axis_index("wide")
    mine = lax.axis_index("narrow")
    z, p = me // plane, me % plane
    pa, pb = pl.ds(0, part), pl.ds(part, chunks - part)

    def at(zz, pp):
        return ((zz + layers) % layers) * plane + (pp + plane) % plane

    zs, ps = range(1, layers), range(1, plane)
    started = []

    def send(src, dst, sem, target):
        copy = pltpu.make_async_remote_copy(
            src_ref=src, dst_ref=dst, send_sem=ssem.at[len(started)], recv_sem=sem,
            device_id=target, device_id_type=MESH)
        copy.start()
        started.append(copy)

    def arrived(dst, sem):
        pltpu.make_async_remote_copy(
            src_ref=dst, dst_ref=dst, send_sem=ssem.at[0], recv_sem=sem,
            device_id={"wide": at(z, p + 1)}, device_id_type=MESH).wait_recv()

    barrier = pltpu.get_barrier_semaphore()
    friends = [{"wide": at(z + d, p)} for d in zs] + [{"wide": at(z, p + d)} for d in ps]
    for back in range(1, reach + 1):
        friends += [{"wide": (me + back) % n}, {"wide": (me + n - back) % n}]
    friends += [{"narrow": (mine + d) % width} for d in range(1, width)]
    for friend in friends:
        pl.semaphore_signal(barrier, inc=1, device_id=friend, device_id_type=MESH)
    pl.semaphore_wait(barrier, len(friends))

    def gather_start(own, buf, sem):
        for d in zs:
            send(own.at[pa], buf.at[me, pa], sem.at[0, me], {"wide": at(z + d, p)})
        for d in ps:
            send(own.at[pb], buf.at[me, pb], sem.at[1, me], {"wide": at(z, p + d)})
        for d in ps:
            send(own.at[pa], buf.at[me, pa], sem.at[0, me], {"wide": at(z, p + d)})
        for d in zs:
            send(own.at[pb], buf.at[me, pb], sem.at[1, me], {"wide": at(z + d, p)})

    def gather_finish(buf, sem):
        for d in range(1, max(layers, plane)):
            if d < layers:
                j = at(z - d, p)
                arrived(buf.at[j, pa], sem.at[0, j])
                for e in ps:
                    send(buf.at[j, pa], buf.at[j, pa], sem.at[0, j], {"wide": at(z, p + e)})
            if d < plane:
                j = at(z, p - d)
                arrived(buf.at[j, pb], sem.at[1, j])
                for e in zs:
                    send(buf.at[j, pb], buf.at[j, pb], sem.at[1, j], {"wide": at(z + e, p)})
        for dz in range(layers):
            for dp in range(plane):
                j = at(z - dz, p - dp)
                if dp:
                    arrived(buf.at[j, pa], sem.at[0, j])
                if dz:
                    arrived(buf.at[j, pb], sem.at[1, j])

    def place(buf, dst):
        for j in range(n):
            for c in range(chunks):
                lane = (c % per) * LANES
                dst[c // per, j * rows:(j + 1) * rows, lane:lane + LANES] = buf[j, c]

    def attend(c):
        def head(h, carry):
            lane = pl.ds(pl.multiple_of(h * ATT, ATT), ATT)
            keys, values, live = [], [], []
            for back in range(reach, 0, -1):
                wraps = jnp.where(me >= back, 0, 1)
                source = (c + groups - wraps) % groups
                keys.append(halo[back - 1, 0, source, :, lane])
                values.append(halo[back - 1, 1, source, :, lane])
            keys.append(qkv[1, c, :, lane])
            values.append(qkv[2, c, :, lane])
            keys, values = jnp.concatenate(keys, axis=0), jnp.concatenate(values, axis=0)
            span = keys.shape[0]
            scores = contract(qkv[0, c, :, lane], keys, 1, 1, lax.Precision.HIGHEST)
            scores = scores / math.sqrt(ATT)
            spot = lax.broadcasted_iota(jnp.int32, (tok, span), 1) - reach * tok
            distance = lax.broadcasted_iota(jnp.int32, (tok, span), 0) - spot
            first = -(c * n + me) * tok
            allowed = (distance >= 0) & (distance < WINDOW) & (spot >= first)
            scores = jnp.where(allowed, scores, -1e30)
            weights = jnp.exp(scores - jnp.max(scores, axis=-1, keepdims=True))
            weights = weights / jnp.sum(weights, axis=-1, keepdims=True)
            mixed[c, :, lane] = contract(weights, values, 1, 0, lax.Precision.HIGHEST)
            return carry

        lax.fori_loop(0, columns // ATT, head, 0)

    def read(value):
        gate, up = times(value, whi, wlo, 0), times(value, whi, wlo, 1)
        return times(gate / (1.0 + jnp.exp(-gate)) * up, whi, wlo, 2, 1)

    def share(c, readout):
        total = jnp.sum(readout * readout, axis=-1, keepdims=True)
        squares[c, mine] = jnp.broadcast_to(total, (tok, LANES))
        for d in range(1, width):
            send(squares.at[c, mine], squares.at[c, mine], qsem.at[c, mine],
                 {"narrow": (mine + d) % width})

    def mix(c, readout):
        for d in range(1, width):
            other = (mine + d) % width
            arrived(squares.at[c, other], qsem.at[c, other])
        total = squares[c, 0]
        for d in range(1, width):
            total = total + squares[c, d]
        scale = jnp.sqrt(total[:, :1] / (columns * width) + EPSILON)
        mixed[c] = mixed[c] + gain[...] * (readout / scale)

    gather_start(own_w, wg, wsem)
    wg[me] = own_w[...]
    gather_finish(wg, wsem)
    for back in range(1, reach + 1):
        for kind in range(2):
            send(qkv.at[1 + kind], halo.at[back - 1, kind], hsem.at[back - 1, kind],
                 {"wide": (me + back) % n})
    place(wg, wfull)
    for m in range(3):
        whi[m], wlo[m] = split(wfull[m])

    key_rows = qkv[1, 0]
    gate, up = times(key_rows, whi, wlo, 0), times(key_rows, whi, wlo, 1)
    sigmoid = 1.0 / (1.0 + jnp.exp(-gate))
    gated = gate * sigmoid
    weighted = eta[...] * qkv[2, 0]
    back_rows = -times(weighted, whi, wlo, 2)
    gate_back = back_rows * up * sigmoid * (1.0 + gate * (1.0 - sigmoid))
    sums = ((key_rows, gate_back), (key_rows, back_rows * gated), (-weighted, gated * up))
    for m, (left, right) in enumerate(sums):
        total = token_sum(left, right)
        for c in range(per):
            for j in range(n):
                grad[j, m * per + c] = total[j * rows:(j + 1) * rows, c * LANES:(c + 1) * LANES]

    for d in range(1, max(layers, plane)):
        if d < plane:
            for e in range(1, layers + 1):
                zz = (z + e) % layers
                send(grad.at[at(zz, p + d), pa], ra.at[d - 1, zz], a1.at[d - 1, zz],
                     {"wide": at(z, p + d)})
        if d < layers:
            for e in range(1, plane + 1):
                pp = (p + e) % plane
                send(grad.at[at(z + d, pp), pb], rb.at[d - 1, pp], b1.at[d - 1, pp],
                     {"wide": at(z + d, p)})

    for back in range(reach):
        for kind in range(2):
            arrived(halo.at[back, kind], hsem.at[back, kind])
    attend(0)

    def half_a(zz):
        total = grad[at(zz, p), pa]
        for d in ps:
            arrived(ra.at[d - 1, zz], a1.at[d - 1, zz])
            total = total + ra[d - 1, zz]
        return total

    def half_b(pp):
        total = grad[at(z, pp), pb]
        for d in zs:
            arrived(rb.at[d - 1, pp], b1.at[d - 1, pp])
            total = total + rb[d - 1, pp]
        return total

    for d in range(1, max(layers, plane)):
        if d < layers:
            sa[d - 1] = half_a((z + d) % layers)
        if d < plane:
            sb[d - 1] = half_b((p + d) % plane)
        if d < layers:
            send(sa.at[d - 1], ra2.at[d - 1], a2.at[d - 1], {"wide": at(z + d, p)})
        if d < plane:
            send(sb.at[d - 1], rb2.at[d - 1], b2.at[d - 1], {"wide": at(z, p + d)})
    new_m[pa] = MOMENTUM_RATE * own_m[pa] + half_a(z)
    new_m[pb] = MOMENTUM_RATE * own_m[pb] + half_b(p)
    for g in range(1, groups):
        attend(g)
    for d in zs:
        arrived(ra2.at[d - 1], a2.at[d - 1])
        new_m[pa] = new_m[pa] + ra2[d - 1]
    for d in ps:
        arrived(rb2.at[d - 1], b2.at[d - 1])
        new_m[pb] = new_m[pb] + rb2[d - 1]
    mg[me] = new_m[...]

    gather_start(new_m, mg, msem)
    first_read = read(qkv[0, 0])
    read0[...] = first_read
    share(0, first_read)
    gather_finish(mg, msem)
    mix(0, read0[...])

    for m in range(3):
        for c in range(m * per, (m + 1) * per):
            lane = pl.ds((c % per) * LANES, LANES)
            weights = wfull[m, :, lane]
            moment = mg[:, c]
            spread = jnp.sqrt(jnp.sum(jnp.sum(moment * moment, axis=0), axis=0, keepdims=True)
                              / columns + EPSILON)
            pull = STEP_SIZE / spread
            stay = wg[:, c] - moment * pull[None]
            ratio = jnp.sqrt(jnp.mean(weights * weights, axis=0, keepdims=True) + EPSILON)
            ratio = ratio / jnp.sqrt(
                jnp.sum(jnp.sum(stay * stay, axis=0), axis=0, keepdims=True) / columns + EPSILON)
            new_w[c] = (own_w[c] - new_m[c] * pull) * ratio
            for j in range(n):
                moved = (wg[j, c] - mg[j, c] * pull) * ratio
                wfull[m, j * rows:(j + 1) * rows, lane] = moved
        whi[m], wlo[m] = split(wfull[m])
    for g in range(1, groups):
        later = read(qkv[0, g])
        share(g, later)
        mix(g, later)
    for copy in started:
        copy.wait_send()


def local(n, width, qkv, eta, fast_weights, momentum, ttt_gain):
    groups, tok, columns = qkv.shape[1:]
    _, rows, three, hidden = fast_weights.shape
    per = hidden // LANES
    chunks = three * per
    part = (chunks + 1) // 2
    rest = chunks - part
    plane = 4 if n % 4 == 0 else 1
    layers = n // plane
    reach = (WINDOW + tok - 2) // tok

    def blocks(value):
        value = value[0].reshape(rows, chunks, LANES)
        return jnp.transpose(value, (1, 0, 2))

    def unblocks(value):
        return jnp.transpose(value, (1, 0, 2)).reshape(1, rows, three, hidden)

    zs, ps = layers - 1, plane - 1
    sends = 2 * (zs + ps + 2 * zs * ps) + 2 * zs + 2 * ps
    sends += ps * layers + zs * plane + zs + ps + 2 * reach + groups * (width - 1)
    vmem, dma = pltpu.VMEM, pltpu.SemaphoreType.DMA
    block = jax.ShapeDtypeStruct((chunks, rows, LANES), F32)
    mixed, new_w, new_m = pl.pallas_call(
        functools.partial(kernel, n, plane, width, part, reach),
        out_shape=(jax.ShapeDtypeStruct((groups, tok, columns), F32), block, block),
        in_specs=[pl.BlockSpec(memory_space=vmem)] * 5,
        out_specs=(pl.BlockSpec(memory_space=vmem),) * 3,
        scratch_shapes=[
            vmem((n, chunks, rows, LANES), F32),
            vmem((n, chunks, rows, LANES), F32),
            vmem((n, chunks, rows, LANES), F32),
            vmem((ps, layers, part, rows, LANES), F32),
            vmem((zs, plane, rest, rows, LANES), F32),
            vmem((zs, part, rows, LANES), F32),
            vmem((ps, rest, rows, LANES), F32),
            vmem((zs, part, rows, LANES), F32),
            vmem((ps, rest, rows, LANES), F32),
            vmem((3, columns, hidden), F32),
            vmem((3, columns, hidden), BF16),
            vmem((3, columns, hidden), BF16),
            vmem((reach, 2, groups, tok, columns), F32),
            vmem((groups, width, tok, LANES), F32),
            vmem((tok, columns), F32),
            dma((2, n)), dma((2, n)),
            dma((ps, layers)), dma((zs, plane)), dma((zs,)), dma((ps,)),
            dma((reach, 2)), dma((groups, width)), dma((sends,)),
        ],
        compiler_params=pltpu.CompilerParams(
            collective_id=0, has_side_effects=True, vmem_limit_bytes=60 * 1024 * 1024),
    )(qkv, eta.reshape(tok, 1), blocks(fast_weights), blocks(momentum),
      ttt_gain.reshape(1, columns))
    return mixed, unblocks(new_w), unblocks(new_m)


def solution(mesh):
    return jax.shard_map(
        functools.partial(local, mesh.shape["wide"], mesh.shape["narrow"]),
        mesh=mesh,
        in_specs=(
            P(None, None, "wide", "narrow"),
            P("narrow", "wide"),
            P("narrow", "wide", None, None),
            P("narrow", "wide", None, None),
            P("narrow"),
        ),
        out_specs=(
            P(None, "wide", "narrow"),
            P("narrow", "wide", None, None),
            P("narrow", "wide", None, None),
        ),
        check_vma=False,
    )
```

```python
import functools
import math

import jax
import jax.numpy as jnp
from jax import lax
from jax.experimental import pallas as pl
from jax.experimental.pallas import tpu as pltpu
from jax.sharding import PartitionSpec as P

ATT = 128
WINDOW = 128
LANES = 128
EPSILON = 1e-06
MOMENTUM_RATE = 0.9
STEP_SIZE = 0.03
MESH = pl.DeviceIdType.MESH
F32 = jnp.float32
BF16 = jnp.bfloat16


def contract(left, right, on_left, on_right, precision=None):
    dims = (((on_left,), (on_right,)), ((), ()))
    return lax.dot_general(left, right, dims, precision=precision, preferred_element_type=F32)


def split(value):
    high = value.astype(BF16)
    return high, (value - high.astype(F32)).astype(BF16)


def times(value, high_ref, low_ref, which, on=0):
    rows = value.shape[0]
    high, low = split(value)
    both = contract(jnp.concatenate([high, low], axis=0), high_ref[which], 1, on)
    return both[:rows] + both[rows:] + contract(high, low_ref[which], 1, on)


def token_sum(left, right):
    high = left.astype(BF16).astype(F32)
    stacked = jnp.concatenate([high, high, left - high], axis=0).T.astype(BF16)
    right_high, right_low = split(right)
    return contract(stacked, jnp.concatenate([right_high, right_low, right_high], axis=0), 1, 0)


def kernel(n, plane, width, part, reach, qkv, eta, own_w, own_m, gain, mixed, new_w, new_m,
           wg, mg, grad, ra, rb, sa, sb, ra2, rb2, wfull, whi, wlo, halo, squares, read0,
           wsem, msem, a1, b1, a2, b2, hsem, qsem, ssem):
    layers = n // plane
    chunks, rows, _ = own_w.shape
    per = chunks // 3
    groups, tok = qkv.shape[1], qkv.shape[2]
    columns = qkv.shape[3]
    me = lax.axis_index("wide")
    mine = lax.axis_index("narrow")
    z, p = me // plane, me % plane
    pa, pb = pl.ds(0, part), pl.ds(part, chunks - part)

    def at(zz, pp):
        return ((zz + layers) % layers) * plane + (pp + plane) % plane

    zs, ps = range(1, layers), range(1, plane)
    started = []

    def send(src, dst, sem, target):
        copy = pltpu.make_async_remote_copy(
            src_ref=src, dst_ref=dst, send_sem=ssem.at[len(started)], recv_sem=sem,
            device_id=target, device_id_type=MESH)
        copy.start()
        started.append(copy)

    def arrived(dst, sem):
        pltpu.make_async_remote_copy(
            src_ref=dst, dst_ref=dst, send_sem=ssem.at[0], recv_sem=sem,
            device_id={"wide": at(z, p + 1)}, device_id_type=MESH).wait_recv()

    barrier = pltpu.get_barrier_semaphore()
    friends = [{"wide": at(z + d, p)} for d in zs] + [{"wide": at(z, p + d)} for d in ps]
    for back in range(1, reach + 1):
        friends += [{"wide": (me + back) % n}, {"wide": (me + n - back) % n}]
    friends += [{"narrow": (mine + d) % width} for d in range(1, width)]
    for friend in friends:
        pl.semaphore_signal(barrier, inc=1, device_id=friend, device_id_type=MESH)
    pl.semaphore_wait(barrier, len(friends))

    def lend(g):
        for back in range(1, reach + 1):
            send(qkv.at[pl.ds(1, 2), g], halo.at[back - 1, g], hsem.at[back - 1, g],
                 {"wide": (me + back) % n})

    def borrow(g):
        for back in range(reach):
            arrived(halo.at[back, g], hsem.at[back, g])

    def gather_start(own, buf, sem):
        for d in zs:
            send(own.at[pa], buf.at[me, pa], sem.at[0, me], {"wide": at(z + d, p)})
        for d in ps:
            send(own.at[pb], buf.at[me, pb], sem.at[1, me], {"wide": at(z, p + d)})
        for d in ps:
            send(own.at[pa], buf.at[me, pa], sem.at[0, me], {"wide": at(z, p + d)})
        for d in zs:
            send(own.at[pb], buf.at[me, pb], sem.at[1, me], {"wide": at(z + d, p)})

    def gather_finish(buf, sem, after):
        for d in range(1, max(layers, plane)):
            if d < layers:
                j = at(z - d, p)
                arrived(buf.at[j, pa], sem.at[0, j])
                for e in ps:
                    send(buf.at[j, pa], buf.at[j, pa], sem.at[0, j], {"wide": at(z, p + e)})
            if d < plane:
                j = at(z, p - d)
                arrived(buf.at[j, pb], sem.at[1, j])
                for e in zs:
                    send(buf.at[j, pb], buf.at[j, pb], sem.at[1, j], {"wide": at(z + e, p)})
        for g in after:
            lend(g)
        for dz in range(layers):
            for dp in range(plane):
                j = at(z - dz, p - dp)
                if dp:
                    arrived(buf.at[j, pa], sem.at[0, j])
                if dz:
                    arrived(buf.at[j, pb], sem.at[1, j])

    def place(buf, dst):
        for j in range(n):
            for c in range(chunks):
                lane = (c % per) * LANES
                dst[c // per, j * rows:(j + 1) * rows, lane:lane + LANES] = buf[j, c]

    def attend(c):
        def head(h, carry):
            lane = pl.ds(pl.multiple_of(h * ATT, ATT), ATT)
            keys, values, live = [], [], []
            for back in range(reach, 0, -1):
                wraps = jnp.where(me >= back, 0, min(c, 1))
                source = c - wraps
                keys.append(halo[back - 1, source, 0, :, lane])
                values.append(halo[back - 1, source, 1, :, lane])
            keys.append(qkv[1, c, :, lane])
            values.append(qkv[2, c, :, lane])
            keys, values = jnp.concatenate(keys, axis=0), jnp.concatenate(values, axis=0)
            span = keys.shape[0]
            scores = contract(qkv[0, c, :, lane], keys, 1, 1, lax.Precision.HIGHEST)
            scores = scores / math.sqrt(ATT)
            spot = lax.broadcasted_iota(jnp.int32, (tok, span), 1) - reach * tok
            distance = lax.broadcasted_iota(jnp.int32, (tok, span), 0) - spot
            first = -(c * n + me) * tok
            allowed = (distance >= 0) & (distance < WINDOW) & (spot >= first)
            scores = jnp.where(allowed, scores, -1e30)
            weights = jnp.exp(scores - jnp.max(scores, axis=-1, keepdims=True))
            weights = weights / jnp.sum(weights, axis=-1, keepdims=True)
            mixed[c, :, lane] = contract(weights, values, 1, 0, lax.Precision.HIGHEST)
            return carry

        lax.fori_loop(0, columns // ATT, head, 0)

    def read(value):
        gate, up = times(value, whi, wlo, 0), times(value, whi, wlo, 1)
        return times(gate / (1.0 + jnp.exp(-gate)) * up, whi, wlo, 2, 1)

    def share(c, readout):
        total = jnp.sum(readout * readout, axis=-1, keepdims=True)
        squares[c, mine] = jnp.broadcast_to(total, (tok, LANES))
        for d in range(1, width):
            send(squares.at[c, mine], squares.at[c, mine], qsem.at[c, mine],
                 {"narrow": (mine + d) % width})

    def mix(c, readout):
        for d in range(1, width):
            other = (mine + d) % width
            arrived(squares.at[c, other], qsem.at[c, other])
        total = squares[c, 0]
        for d in range(1, width):
            total = total + squares[c, d]
        scale = jnp.sqrt(total[:, :1] / (columns * width) + EPSILON)
        mixed[c] = mixed[c] + gain[...] * (readout / scale)

    gather_start(own_w, wg, wsem)
    wg[me] = own_w[...]
    gather_finish(wg, wsem, (0,))
    place(wg, wfull)
    for m in range(3):
        whi[m], wlo[m] = split(wfull[m])

    key_rows = qkv[1, 0]
    gate, up = times(key_rows, whi, wlo, 0), times(key_rows, whi, wlo, 1)
    sigmoid = 1.0 / (1.0 + jnp.exp(-gate))
    gated = gate * sigmoid
    weighted = eta[...] * qkv[2, 0]
    back_rows = -times(weighted, whi, wlo, 2)
    gate_back = back_rows * up * sigmoid * (1.0 + gate * (1.0 - sigmoid))
    sums = ((key_rows, gate_back), (key_rows, back_rows * gated), (-weighted, gated * up))
    for m, (left, right) in enumerate(sums):
        total = token_sum(left, right)
        for c in range(per):
            for j in range(n):
                grad[j, m * per + c] = total[j * rows:(j + 1) * rows, c * LANES:(c + 1) * LANES]

    for d in range(1, max(layers, plane)):
        if d < plane:
            for e in range(1, layers + 1):
                zz = (z + e) % layers
                send(grad.at[at(zz, p + d), pa], ra.at[d - 1, zz], a1.at[d - 1, zz],
                     {"wide": at(z, p + d)})
        if d < layers:
            for e in range(1, plane + 1):
                pp = (p + e) % plane
                send(grad.at[at(z + d, pp), pb], rb.at[d - 1, pp], b1.at[d - 1, pp],
                     {"wide": at(z + d, p)})

    borrow(0)
    attend(0)

    def half_a(zz):
        total = grad[at(zz, p), pa]
        for d in ps:
            arrived(ra.at[d - 1, zz], a1.at[d - 1, zz])
            total = total + ra[d - 1, zz]
        return total

    def half_b(pp):
        total = grad[at(z, pp), pb]
        for d in zs:
            arrived(rb.at[d - 1, pp], b1.at[d - 1, pp])
            total = total + rb[d - 1, pp]
        return total

    for d in range(1, max(layers, plane)):
        if d < layers:
            sa[d - 1] = half_a((z + d) % layers)
        if d < plane:
            sb[d - 1] = half_b((p + d) % plane)
        if d < layers:
            send(sa.at[d - 1], ra2.at[d - 1], a2.at[d - 1], {"wide": at(z + d, p)})
        if d < plane:
            send(sb.at[d - 1], rb2.at[d - 1], b2.at[d - 1], {"wide": at(z, p + d)})
    new_m[pa] = MOMENTUM_RATE * own_m[pa] + half_a(z)
    new_m[pb] = MOMENTUM_RATE * own_m[pb] + half_b(p)
    for d in zs:
        arrived(ra2.at[d - 1], a2.at[d - 1])
        new_m[pa] = new_m[pa] + ra2[d - 1]
    for d in ps:
        arrived(rb2.at[d - 1], b2.at[d - 1])
        new_m[pb] = new_m[pb] + rb2[d - 1]
    mg[me] = new_m[...]

    gather_start(new_m, mg, msem)
    first_read = read(qkv[0, 0])
    read0[...] = first_read
    share(0, first_read)
    gather_finish(mg, msem, range(1, groups))
    mix(0, read0[...])

    for m in range(3):
        for c in range(m * per, (m + 1) * per):
            lane = pl.ds((c % per) * LANES, LANES)
            weights = wfull[m, :, lane]
            moment = mg[:, c]
            spread = jnp.sqrt(jnp.sum(jnp.sum(moment * moment, axis=0), axis=0, keepdims=True)
                              / columns + EPSILON)
            pull = STEP_SIZE / spread
            stay = wg[:, c] - moment * pull[None]
            ratio = jnp.sqrt(jnp.mean(weights * weights, axis=0, keepdims=True) + EPSILON)
            ratio = ratio / jnp.sqrt(
                jnp.sum(jnp.sum(stay * stay, axis=0), axis=0, keepdims=True) / columns + EPSILON)
            new_w[c] = (own_w[c] - new_m[c] * pull) * ratio
            for j in range(n):
                moved = (wg[j, c] - mg[j, c] * pull) * ratio
                wfull[m, j * rows:(j + 1) * rows, lane] = moved
        whi[m], wlo[m] = split(wfull[m])
    for g in range(1, groups):
        later = read(qkv[0, g])
        share(g, later)
        borrow(g)
        attend(g)
        mix(g, later)
    for copy in started:
        copy.wait_send()


def local(n, width, qkv, eta, fast_weights, momentum, ttt_gain):
    groups, tok, columns = qkv.shape[1:]
    _, rows, three, hidden = fast_weights.shape
    per = hidden // LANES
    chunks = three * per
    part = 7 * chunks // 9
    rest = chunks - part
    plane = 4 if n % 4 == 0 else 1
    layers = n // plane
    reach = (WINDOW + tok - 2) // tok

    def blocks(value):
        value = value[0].reshape(rows, chunks, LANES)
        return jnp.transpose(value, (1, 0, 2))

    def unblocks(value):
        return jnp.transpose(value, (1, 0, 2)).reshape(1, rows, three, hidden)

    zs, ps = layers - 1, plane - 1
    sends = 2 * (zs + ps + 2 * zs * ps) + 2 * zs + 2 * ps
    sends += ps * layers + zs * plane + zs + ps + groups * reach + groups * (width - 1)
    vmem, dma = pltpu.VMEM, pltpu.SemaphoreType.DMA
    block = jax.ShapeDtypeStruct((chunks, rows, LANES), F32)
    mixed, new_w, new_m = pl.pallas_call(
        functools.partial(kernel, n, plane, width, part, reach),
        out_shape=(jax.ShapeDtypeStruct((groups, tok, columns), F32), block, block),
        in_specs=[pl.BlockSpec(memory_space=vmem)] * 5,
        out_specs=(pl.BlockSpec(memory_space=vmem),) * 3,
        scratch_shapes=[
            vmem((n, chunks, rows, LANES), F32),
            vmem((n, chunks, rows, LANES), F32),
            vmem((n, chunks, rows, LANES), F32),
            vmem((ps, layers, part, rows, LANES), F32),
            vmem((zs, plane, rest, rows, LANES), F32),
            vmem((zs, part, rows, LANES), F32),
            vmem((ps, rest, rows, LANES), F32),
            vmem((zs, part, rows, LANES), F32),
            vmem((ps, rest, rows, LANES), F32),
            vmem((3, columns, hidden), F32),
            vmem((3, columns, hidden), BF16),
            vmem((3, columns, hidden), BF16),
            vmem((reach, groups, 2, tok, columns), F32),
            vmem((groups, width, tok, LANES), F32),
            vmem((tok, columns), F32),
            dma((2, n)), dma((2, n)),
            dma((ps, layers)), dma((zs, plane)), dma((zs,)), dma((ps,)),
            dma((reach, groups)), dma((groups, width)), dma((sends,)),
        ],
        compiler_params=pltpu.CompilerParams(
            collective_id=0, has_side_effects=True, vmem_limit_bytes=60 * 1024 * 1024),
    )(qkv, eta.reshape(tok, 1), blocks(fast_weights), blocks(momentum),
      ttt_gain.reshape(1, columns))
    return mixed, unblocks(new_w), unblocks(new_m)


def solution(mesh):
    return jax.shard_map(
        functools.partial(local, mesh.shape["wide"], mesh.shape["narrow"]),
        mesh=mesh,
        in_specs=(
            P(None, None, "wide", "narrow"),
            P("narrow", "wide"),
            P("narrow", "wide", None, None),
            P("narrow", "wide", None, None),
            P("narrow"),
        ),
        out_specs=(
            P(None, "wide", "narrow"),
            P("narrow", "wide", None, None),
            P("narrow", "wide", None, None),
        ),
        check_vma=False,
    )
```
